32 devices in a mesh: row: 8 (over z, y), col: 4 (over x, core).
Axes of the slice: x: 2, y: 2, z: 4, core: 2. Of those that a mesh axis runs over, the one named last changes fastest.
Arguments:
- density: bfloat16 [32, 12, 256, 256], P('row', 'col'), may hold values from -0.75 to 0.75
- col_list: int32 [32, 12], replicated, may hold values from 0 to 31, as said below
- orbital_position: bfloat16 [32, 3, 256], P('row'), may hold values from 0 to 1
- orbital_exponent: bfloat16 [32, 256], P('row'), may hold values from 0.019897461 to 3
- row_tiles: int32 [32, 6], P('row'), may hold values from 0 to 63, as said below
- tile_counts: int32 [8], replicated, may hold values from 0 to 16, as said below
- point_offset: bfloat16 [64, 3, 1024], replicated, may hold values from 0 to 1
- core_density: float32 [128, 1024], P('row', 'col'), may hold values from 0.025 to 8
- quad_weight: float32 [128, 1024], P('row', 'col'), may hold values from 0.2 to 2
Outputs:
- new_density: bfloat16 [32, 12, 256, 256], P('row', 'col')
- ks_blocks: float32 [32, 12, 256, 256], P('row', 'col')
- valence: float32 [128, 1024], P('row', 'col')
The draws below stay inside these ranges and needn't reach their ends.
Inputs may be any that keep to these rules, and one draw needn't show every extreme that they name: `col_list`: entries g * 3 to g * 3 + 2 of block row a are 3 distinct block columns b with b modulo (4) equal to g, each within 8 of a cyclically modulo 32, in increasing order of the signed distance from a; a itself is listed. `row_tiles`: block row a lists 6 distinct tiles among 2 * a - 3 to 2 * a + 4 taken modulo 64, in increasing order of that offset. `tile_counts`: indices 2 * p and 2 * p + 1 of row together own the 16 tiles from 16 * p on; each index owns consecutive tiles, lower indices first; some index owns 16.
All inputs are finite; a program needn't handle non-finite values.
Results may differ from the reference program's by a relative error of at most 0.006.
Values may be sent and summed in bfloat16 or wider, within the bound.
A program may use at most 128 MiB of HBM per device.

```python
import math
import jax
import jax.numpy as jnp
from jax import lax

B = 256
K = 12
BAND = 8
G = 1024
TROW = 6
RDEV = 4
KG = 3
NB = 32
NT = 64
TCAP = 16
TSLOTS = 128


def draw_col_list(key, part):
    row_ids = jnp.arange(NB, dtype=jnp.int32)
    offsets = jnp.arange(-BAND, BAND + 1, dtype=jnp.int32)
    window_size = 2 * BAND + 1
    random_bits = jax.random.randint(key, (NB, window_size), 0, 2 ** 20, dtype=jnp.int32)
    scores = random_bits * 32 + jnp.arange(window_size, dtype=jnp.int32)[None, :]
    scores = jnp.where(offsets[None, :] == 0, 2 ** 30, scores)
    columns = jnp.mod(row_ids[:, None] + offsets[None, :], NB)
    residue = jnp.mod(columns, K // KG)
    pieces = []
    for group_id in range(K // KG):
        masked = jnp.where(residue == group_id, scores, -1)
        winners = lax.top_k(masked, KG)[1]
        chosen = jnp.sort(jnp.take(offsets, winners), axis=1)
        pieces.append(jnp.mod(row_ids[:, None] + chosen, NB))
    return jnp.concatenate(pieces, axis=1).astype(jnp.int32)


def draw_row_tiles(key, part):
    row_ids = jnp.arange(NB, dtype=jnp.int32)
    random_bits = jax.random.randint(key, (NB, 8), 0, 2 ** 20, dtype=jnp.int32) * 8 + jnp.arange(8, dtype=jnp.int32)[None, :]
    winners = jnp.sort(lax.top_k(random_bits, TROW)[1], axis=1).astype(jnp.int32)
    return jnp.mod(2 * row_ids[:, None] - 3 + winners, NT).astype(jnp.int32)


def draw_tile_counts(key, part):
    pair_count = NB // RDEV // 2
    first_share = jax.random.randint(jax.random.fold_in(key, 1), (pair_count,), 0, TCAP + 1, dtype=jnp.int32)
    forced = jax.random.randint(jax.random.fold_in(key, 2), (), 0, pair_count, dtype=jnp.int32)
    first_share = jnp.where(jnp.arange(pair_count, dtype=jnp.int32) == forced, TCAP, first_share)
    return jnp.stack([first_share, TCAP - first_share], axis=1).reshape(2 * pair_count).astype(jnp.int32)


def draw_core_density(key, part):
    levels = jnp.exp(jax.random.uniform(jax.random.fold_in(key, 11), (TSLOTS, 1), jnp.float32, math.log(0.05), math.log(4.0)))
    detail = jnp.exp(jax.random.uniform(jax.random.fold_in(key, 12), (TSLOTS, G), jnp.float32, math.log(0.5), math.log(2.0)))
    return (levels * detail).astype(jnp.float32)


def block_levels(rng, shape, cuts, least, largest):
    gain = 1.0
    for axis_at, parts in cuts:
        steps = jax.random.uniform(jax.random.fold_in(jax.random.fold_in(rng, 6), axis_at), (parts,), jnp.float32, least / len(cuts), largest / len(cuts))
        gain = gain * jnp.repeat(jnp.exp(steps), shape[axis_at] // parts).reshape((-1,) + (1,) * (len(shape) - 1 - axis_at))
    return gain


def centred(key, shape, width, bound, cuts=(), held_as=jnp.bfloat16):
    drawn = width * jax.random.normal(key, shape, jnp.float32)
    if cuts:
        drawn = drawn * block_levels(key, shape, cuts, -0.22, 0.18)
    return jnp.clip(drawn, -bound, bound).astype(held_as)


def setup_inputs(seed: int = 0) -> dict:
    key_list = jax.random.split(jax.random.key(seed), 10)
    return {
        "density": centred(key_list[0], (NB, K, B, B), (B // 4) ** -0.5, 0.75, ((0, 8), (1, 4))),
        "col_list": draw_col_list(jax.random.fold_in(key_list[9], 71), 0),
        "orbital_position": jnp.clip(1.0 * jax.random.uniform(key_list[2], (NB, 3, B), jnp.float32) ** block_levels(key_list[2], (NB, 3, B), ((0, 8),), -0.2, 0.2), 0.0, 1.0).astype(jnp.bfloat16),
        "orbital_exponent": jnp.clip(jnp.exp(math.log(3.0) - 5.015775 * jax.random.uniform(key_list[3], (NB, B), jnp.float32) ** block_levels(key_list[3], (NB, B), ((0, 8),), -0.2, 0.2)), 0.019897461, 3.0).astype(jnp.bfloat16),
        "row_tiles": draw_row_tiles(jax.random.fold_in(key_list[9], 71), 0),
        "tile_counts": draw_tile_counts(jax.random.fold_in(key_list[9], 71), 0),
        "point_offset": jnp.clip(jax.random.uniform(key_list[6], (NT, 3, G), jnp.float32, 0.0, 1.0), 0.0, 1.0).astype(jnp.bfloat16),
        "core_density": draw_core_density(jax.random.fold_in(key_list[9], 71), 0),
        "quad_weight": jnp.clip(jnp.exp(math.log(2.0) - 2.3025851 * jax.random.uniform(key_list[8], (TSLOTS, G), jnp.float32) ** block_levels(key_list[8], (TSLOTS, G), ((0, 8), (1, 4)), -0.2, 0.2)), 0.2, 2.0),
    }


SLATER = 0.9847450218426965

def basis_values(position, exponent, home_row, tile_id, tile_points, period):
    grid_x = tile_id.astype(jnp.float32) + tile_points[0]
    centre_x = 2.0 * home_row.astype(jnp.float32) + 2.0 * position[0]
    delta_x = jnp.mod(grid_x[None, :] - centre_x[:, None] + 0.5 * period, period) - 0.5 * period
    delta_y = tile_points[1][None, :] - position[1][:, None]
    delta_z = tile_points[2][None, :] - position[2][:, None]
    radius = delta_x * delta_x + delta_y * delta_y + delta_z * delta_z
    scaling = 1.0 / math.sqrt(position.shape[-1])
    return (jnp.exp(-exponent[:, None] * radius) * scaling).astype(jnp.bfloat16)

def potential(valence, core, weight):
    amount = core + jax.nn.softplus(valence)
    return weight * (-SLATER * jnp.cbrt(amount)) * jax.nn.sigmoid(valence)

def reference(density, col_list, orbital_position, orbital_exponent, row_tiles, tile_counts, point_offset, core_density, quad_weight):
    highest = lax.Precision.HIGHEST
    position = orbital_position.astype(jnp.float32)
    exponent = orbital_exponent.astype(jnp.float32)
    points = point_offset.astype(jnp.float32)
    period = 1.0 * NT
    row_ids = jnp.arange(NB, dtype=jnp.int32)

    def square_row(row_id):
        neighbours = col_list[row_id]
        left_side = density[row_id].astype(jnp.float32)
        right_side = density[neighbours].astype(jnp.float32)
        matches = (col_list[neighbours][:, :, None] == neighbours[None, None, :]).astype(jnp.float32)
        chosen = jnp.einsum('mlk,mlxy->kmxy', matches, right_side, precision=highest)
        return jnp.einsum('mxz,kmzy->kxy', left_side, chosen, precision=highest)
    square = lax.map(square_row, row_ids)
    new_density = (2.0 * density.astype(jnp.float32) - square).astype(jnp.bfloat16)
    new_wide = lax.optimization_barrier(new_density).astype(jnp.float32)

    def row_basis(row_id, tile_id):
        tile_points = points[tile_id]
        own_basis = basis_values(position[row_id], exponent[row_id], row_id, tile_id, tile_points, period)
        neighbours = col_list[row_id]
        others = jax.vmap(lambda column: basis_values(position[column], exponent[column], column, tile_id, tile_points, period))(neighbours)
        own_basis, others = lax.optimization_barrier((own_basis, others))
        return (own_basis.astype(jnp.float32), others.astype(jnp.float32))

    def collocate_row(row_id):
        blocks = new_wide[row_id]

        def per_tile(tile_id):
            own_basis, others = row_basis(row_id, tile_id)
            mixture = jnp.einsum('kxy,kyg->xg', blocks, others, precision=highest)
            return lax.optimization_barrier(jnp.sum(own_basis * mixture, axis=0))
        return lax.map(per_tile, row_tiles[row_id])
    partial_value = lax.map(collocate_row, row_ids)
    flat_tiles = row_tiles.reshape(-1)
    tile_hits = (flat_tiles[:, None] == jnp.arange(NT, dtype=jnp.int32)[None, :]).astype(jnp.float32)
    tile_density = jnp.dot(tile_hits.T, partial_value.reshape(-1, G), precision=highest)
    upper_ends = jnp.cumsum(tile_counts).astype(jnp.int32)
    starts = upper_ends - tile_counts
    slot_ids = jnp.arange(TCAP, dtype=jnp.int32)
    occupied = slot_ids[None, :] < tile_counts[:, None]
    slot_tiles = jnp.where(occupied, starts[:, None] + slot_ids[None, :], 0).reshape(-1)
    valence = jnp.where(occupied.reshape(-1)[:, None], tile_density[slot_tiles], 0.0)
    field_slots = potential(valence, core_density, quad_weight)
    all_tiles = jnp.arange(NT, dtype=jnp.int32)
    owners = lax.optimization_barrier(jnp.sum((upper_ends[None, :] <= all_tiles[:, None]).astype(jnp.int32), axis=1))
    holder = owners * TCAP + all_tiles - starts[owners]
    field_tiles = field_slots[holder]

    def integrate_row(row_id):

        def per_tile(running, tile_id):
            own_basis, others = row_basis(row_id, tile_id)
            weighted = (own_basis * field_tiles[tile_id][None, :]).astype(jnp.bfloat16)
            weighted = lax.optimization_barrier(weighted).astype(jnp.float32)
            update = jnp.einsum('xg,kyg->kxy', weighted, others, precision=highest)
            return (running + update, None)
        running, unused = lax.scan(per_tile, jnp.zeros((K, B, B), jnp.float32), row_tiles[row_id])
        return running
    ks_blocks = lax.map(integrate_row, row_ids)
    return (new_density, ks_blocks, valence)
```

```python
import functools
import math

import jax
import jax.numpy as jnp
from jax import lax
from jax.experimental import pallas as pl
from jax.experimental.pallas import tpu as pltpu
from jax.sharding import PartitionSpec as P

BAND = 8
REACH = 3
SLATER = 0.9847450218426965
LOG2E = 1.4426950408889634


def from_behind(value, axis, steps):
    count = lax.axis_size(axis)
    pairs = [(source, (source + steps) % count) for source in range(count)]
    return lax.ppermute(value, axis, pairs)


def potential(valence, core, weight):
    amount = core + jax.nn.softplus(valence)
    return weight * (-SLATER * jnp.cbrt(amount)) * jax.nn.sigmoid(valence)


def split3(x):
    high = x.astype(jnp.bfloat16).astype(jnp.float32)
    rest = x - high
    mid = rest.astype(jnp.bfloat16).astype(jnp.float32)
    return high, mid, rest - mid


def point_features(pts):
    pts = pts.astype(jnp.float32)
    ox, oy, oz = pts[0:1], pts[1:2], pts[2:3]
    square = ox * ox + oy * oy + oz * oz
    row = lax.broadcasted_iota(jnp.int32, (8, pts.shape[1]), 0)
    feats = jnp.where(row == 0, square, 0.0)
    feats = jnp.where(row == 1, ox, feats)
    feats = jnp.where(row == 2, oy, feats)
    feats = jnp.where(row == 3, oz, feats)
    feats = jnp.where(row == 4, 1.0, feats)
    high, mid, low = split3(feats)
    return jnp.concatenate([high, high, high, mid, mid, low], axis=0).astype(jnp.bfloat16)


def orbital_features(params, shift):
    size = params.shape[1]
    px, py, pz = params[0:1], params[1:2], params[2:3]
    scaled = params[3:4] * LOG2E
    px = 2.0 * px - shift
    row = lax.broadcasted_iota(jnp.int32, (8, size), 0)
    const = -scaled * (px * px + py * py + pz * pz) - 0.5 * math.log2(size)
    feats = jnp.where(row == 0, -scaled, 0.0)
    feats = jnp.where(row == 1, 2.0 * scaled * px, feats)
    feats = jnp.where(row == 2, 2.0 * scaled * py, feats)
    feats = jnp.where(row == 3, 2.0 * scaled * pz, feats)
    feats = jnp.where(row == 4, const, feats)
    high, mid, low = split3(feats)
    return jnp.concatenate([high, mid, low, high, mid, high], axis=0).astype(jnp.bfloat16)


def fill_basis(phi_ref, par_ref, pts_ref, tiles_ref, shift_ref, row, j):
    members, size = par_ref.shape[1], par_ref.shape[3]
    feats = point_features(pts_ref[tiles_ref[row, j]])
    for member in range(members):
        shift = shift_ref[row, j * members + member].astype(jnp.float32)
        coefs = orbital_features(par_ref[0, member], shift)
        expo = lax.dot_general(
            coefs, feats, (((0,), (0,)), ((), ())), preferred_element_type=jnp.float32
        )
        phi_ref[member * size : (member + 1) * size, :] = jnp.exp2(expo).astype(jnp.bfloat16)


def square_kernel(
    pick_ref, tiles_ref, shift_ref, full_ref, par_ref, pts_ref, *rest
):
    pieces = rest[:-6]
    new_ref, part_ref, band, newcat, phi, sem = rest[-6:]
    row = pl.program_id(0)
    groups, kg, size = full_ref.shape[0], full_ref.shape[2], full_ref.shape[3]
    per_piece = pieces[0].shape[0]

    @pl.when(row == 0)
    def _():
        copies = [
            pltpu.make_async_copy(piece, band.at[pl.ds(at * per_piece, per_piece)], sem.at[at])
            for at, piece in enumerate(pieces)
        ]
        for copy in copies:
            copy.start()
        band[len(pieces) * per_piece] = jnp.zeros((size, size), jnp.bfloat16)
        for copy in copies:
            copy.wait()

    own_at = (len(pieces) // 2) * per_piece + row * kg
    for k in range(kg):
        acc = jnp.zeros((size, size), jnp.float32)
        for m in range(groups * kg):
            acc = acc + jnp.dot(
                full_ref[m // kg, 0, m % kg],
                band[pick_ref[row, k * groups * kg + m]],
                preferred_element_type=jnp.float32,
            )
        fresh = (2.0 * band[own_at + k].astype(jnp.float32) - acc).astype(jnp.bfloat16)
        new_ref[0, k] = fresh
        newcat[:, k * size : (k + 1) * size] = fresh

    points = phi.shape[1]

    def step(j, carry):
        fill_basis(phi, par_ref, pts_ref, tiles_ref, shift_ref, row, j)
        for at in range(points // size):
            cols = slice(at * size, (at + 1) * size)
            mix = jnp.dot(newcat[...], phi[size:, cols], preferred_element_type=jnp.float32)
            own = phi[:size, cols].astype(jnp.float32)
            part_ref[0, pl.ds(j, 1), cols] = jnp.sum(own * mix, axis=0, keepdims=True)
        return carry

    lax.fori_loop(0, tiles_ref.shape[1], step, 0)


def ks_kernel(tiles_ref, shift_ref, holder_ref, par_ref, pts_ref, field_ref, out_ref, phi):
    row = pl.program_id(0)
    kg, size = out_ref.shape[1], out_ref.shape[2]
    out_ref[...] = jnp.zeros(out_ref.shape, jnp.float32)

    def step(j, carry):
        fill_basis(phi, par_ref, pts_ref, tiles_ref, shift_ref, row, j)
        field = field_ref[pl.ds(holder_ref[row, j], 1), :]
        weighted = (phi[:size].astype(jnp.float32) * field).astype(jnp.bfloat16)
        for k in range(kg):
            out_ref[0, k] += lax.dot_general(
                weighted,
                phi[(k + 1) * size : (k + 2) * size],
                (((1,), (1,)), ((), ())),
                preferred_element_type=jnp.float32,
            )
        return carry

    lax.fori_loop(0, tiles_ref.shape[1], step, 0)


def body(
    density,
    col_list,
    orbital_position,
    orbital_exponent,
    row_tiles,
    tile_counts,
    point_offset,
    core_density,
    quad_weight,
):
    highest = lax.Precision.HIGHEST
    rows_here, kg, size = density.shape[:3]
    tiles_listed = row_tiles.shape[1]
    blocks_total, neighbours_listed = col_list.shape
    tiles_total, _, points = point_offset.shape
    row_count = lax.axis_size("row")
    groups = lax.axis_size("col")
    row_index = lax.axis_index("row")
    col_index = lax.axis_index("col")
    reach_rows = -(-BAND // rows_here)
    base_row = (row_index - reach_rows) * rows_here
    flat = density.reshape(rows_here * kg, size, size)
    pieces = [
        flat if offset == 0 else from_behind(flat, "row", -offset)
        for offset in range(-reach_rows, reach_rows + 1)
    ]
    full = lax.all_gather(density, "col", axis=0)
    orbitals = jnp.concatenate([orbital_position, orbital_exponent[:, None]], axis=1)
    orbitals = lax.all_gather(orbitals, "row", axis=0, tiled=True)

    row_ids = row_index * rows_here + jnp.arange(rows_here, dtype=jnp.int32)
    lists = lax.dynamic_slice_in_dim(col_list, row_index * rows_here, rows_here, axis=0)
    own_cols = lax.dynamic_slice_in_dim(lists, col_index * kg, kg, axis=1)
    places = jnp.mod(lists - base_row, blocks_total)
    group_lists = lax.dynamic_slice_in_dim(col_list, col_index * kg, kg, axis=1)
    right_cols = jnp.take(group_lists, lists, axis=0)
    matches = right_cols[:, None, :, :] == own_cols[:, :, None, None]
    zero_block = len(pieces) * rows_here * kg
    flat_at = places[:, None, :, None] * kg + jnp.arange(kg, dtype=jnp.int32)
    pick = jnp.min(jnp.where(matches, flat_at, zero_block), axis=-1)
    pick = pick.reshape(rows_here, kg * neighbours_listed)

    members = jnp.concatenate([row_ids[:, None], own_cols], axis=1)
    params = jnp.take(orbitals, members, axis=0).astype(jnp.float32)
    params = jnp.pad(params, ((0, 0), (0, 0), (0, 4), (0, 0)))
    half = tiles_total // 2
    shift = row_tiles[:, :, None] - 2 * members[:, None, :]
    shift = jnp.mod(shift + half, tiles_total) - half
    shift = shift.reshape(rows_here, tiles_listed * (kg + 1))

    whole = lambda shape: pl.BlockSpec(shape, lambda i, *_: (0,) * len(shape))
    par_spec = pl.BlockSpec((1, kg + 1, 8, size), lambda i, *_: (i, 0, 0, 0))
    basis_flops = 2 * rows_here * tiles_listed * (kg + 1) * size * points * size
    new_density, partial = pl.pallas_call(
        square_kernel,
        out_shape=(
            jax.ShapeDtypeStruct(density.shape, jnp.bfloat16),
            jax.ShapeDtypeStruct((rows_here, tiles_listed, points), jnp.float32),
        ),
        grid_spec=pltpu.PrefetchScalarGridSpec(
            num_scalar_prefetch=3,
            grid=(rows_here,),
            in_specs=[
                pl.BlockSpec((groups, 1, kg, size, size), lambda i, *_: (0, i, 0, 0, 0)),
                par_spec,
                whole(point_offset.shape),
            ]
            + [pl.BlockSpec(memory_space=pl.ANY)] * len(pieces),
            out_specs=(
                pl.BlockSpec((1, kg, size, size), lambda i, *_: (i, 0, 0, 0)),
                pl.BlockSpec((1, tiles_listed, points), lambda i, *_: (i, 0, 0)),
            ),
            scratch_shapes=[
                pltpu.VMEM((zero_block + 1, size, size), jnp.bfloat16),
                pltpu.VMEM((size, kg * size), jnp.bfloat16),
                pltpu.VMEM(((kg + 1) * size, points), jnp.bfloat16),
                pltpu.SemaphoreType.DMA((len(pieces),)),
            ],
        ),
        compiler_params=pltpu.CompilerParams(dimension_semantics=("arbitrary",)),
        cost_estimate=pl.CostEstimate(
            flops=2 * basis_flops, bytes_accessed=20_000_000, transcendentals=0
        ),
        name="square_collocate",
    )(pick, row_tiles, shift, full, params, point_offset, *pieces)

    shares = lax.psum_scatter(
        partial.reshape(rows_here * tiles_listed, points), "col", scatter_dimension=1, tiled=True
    )
    reach_tiles = 2 * REACH
    window = -(-(2 * rows_here + reach_tiles) // 8) * 8
    first = 2 * rows_here * row_index - REACH
    spot = jnp.mod(row_tiles.reshape(-1) - first, tiles_total)
    spots = jnp.arange(window, dtype=jnp.int32)
    packed = jnp.dot(
        (spots[:, None] == spot[None, :]).astype(jnp.float32), shares, precision=highest
    )
    gathered = lax.all_gather(packed, "row", axis=0, tiled=True)
    upper_ends = jnp.cumsum(tile_counts)
    starts = upper_ends - tile_counts
    slot_count = core_density.shape[0]
    slots = jnp.arange(slot_count, dtype=jnp.int32)
    my_start = jnp.take(starts, row_index)
    my_tiles = jnp.where(slots < jnp.take(tile_counts, row_index), my_start + slots, -1)
    senders = jnp.arange(row_count, dtype=jnp.int32)
    sent_tiles = jnp.mod(
        (2 * rows_here * senders - REACH)[:, None] + spots[None, :], tiles_total
    ).reshape(-1)
    valence = jnp.dot(
        (my_tiles[:, None] == sent_tiles[None, :]).astype(jnp.float32), gathered, precision=highest
    )
    field = potential(valence, core_density, quad_weight)
    field = lax.all_gather(field, "row", axis=0, tiled=True)
    field = lax.all_gather(field, "col", axis=1, tiled=True)
    owners = jnp.sum((upper_ends <= row_tiles[:, :, None]).astype(jnp.int32), axis=-1)
    holder = owners * slot_count + row_tiles - jnp.take(starts, owners)

    ks = pl.pallas_call(
        ks_kernel,
        out_shape=jax.ShapeDtypeStruct(density.shape, jnp.float32),
        grid_spec=pltpu.PrefetchScalarGridSpec(
            num_scalar_prefetch=3,
            grid=(rows_here,),
            in_specs=[par_spec, whole(point_offset.shape), whole(field.shape)],
            out_specs=pl.BlockSpec((1, kg, size, size), lambda i, *_: (i, 0, 0, 0)),
            scratch_shapes=[pltpu.VMEM(((kg + 1) * size, points), jnp.bfloat16)],
        ),
        compiler_params=pltpu.CompilerParams(dimension_semantics=("arbitrary",)),
        cost_estimate=pl.CostEstimate(
            flops=2 * basis_flops, bytes_accessed=5_000_000, transcendentals=0
        ),
        name="ks_blocks",
    )(row_tiles, shift, holder, params, point_offset, field)
    return (new_density, ks, valence)


def solution(mesh):
    return jax.shard_map(
        body,
        mesh=mesh,
        in_specs=(
            P("row", "col", None, None),
            P(),
            P("row", None, None),
            P("row", None),
            P("row", None),
            P(),
            P(),
            P("row", "col"),
            P("row", "col"),
        ),
        out_specs=(P("row", "col", None, None), P("row", "col", None, None), P("row", "col")),
        check_vma=False,
    )
```
